256 devices in a mesh: bank: 8 (over x, core), zero: 32 (over z, y).
Axes of the slice: x: 4, y: 4, z: 8, core: 2. Of those that a mesh axis runs over, the one named last changes fastest.
Arguments:
- train_gate: float32 [128, 2048, 768], P('bank', 'zero'), may hold values from -0.25 to 0.25
- other_gate: bfloat16 [128, 2048, 768], P('bank', 'zero'), may hold values from -0.0625 to 0.0625
- train_up: float32 [128, 2048, 768], P('bank', 'zero'), may hold values from -0.25 to 0.25
- other_up: bfloat16 [128, 2048, 768], P('bank', 'zero'), may hold values from -0.0625 to 0.0625
- router_weight: float32 [2048, 128], P('zero', 'bank'), may hold values from -0.125 to 0.125
- router_gain: float32 [2048], P('zero'), may hold values from 0.25 to 1.75
Outputs:
- ready_gate: bfloat16 [128, 2048, 768], P('bank', None, 'zero')
- ready_up: bfloat16 [128, 2048, 768], P('bank', None, 'zero')
- scale_gate: float32 [128, 768], P('bank', 'zero')
- scale_up: float32 [128, 768], P('bank', 'zero')
- serve_router: bfloat16 [2048, 128], replicated
The draws below stay inside these ranges and needn't reach their ends.
All inputs are finite; a program needn't handle non-finite values. Where the reference program divides by a largest or mean magnitude, that divisor is 1e-20 or more.
Results may differ from the reference program's by a relative error of at most 0.001.
Values may be sent and summed in bfloat16 or wider, within the bound.
A program may use at most 64 MiB of HBM per device.

```python
import jax
import jax.numpy as jnp

EXPERTS = 128
D_MODEL = 2048
D_EXPERT = 768


def raised(array, rng, source, target, parts, factor):
    owner, partner = [(jnp.arange(array.shape[axis_at]) // (array.shape[axis_at] // parts)).reshape([-1 if axis == axis_at else 1 for axis in range(array.ndim)]) for axis_at in (source, target)]
    chosen = jax.random.permutation(rng, parts)[partner]
    strong = (owner == chosen) | (owner == (partner + parts // 2) % parts)
    return jnp.where(strong, factor * array, array)


def level_of(rng, extent, pieces, smallest, high):
    factor_of, own = 1.0, jax.random.fold_in(rng, 6)
    for position, blocks in pieces:
        draws = jnp.exp(jax.random.uniform(jax.random.fold_in(own, position), (blocks,), jnp.float32, smallest / len(pieces), high / len(pieces)))
        factor_of = factor_of * jnp.repeat(draws, extent[position] // blocks).reshape([-1 if axis == position else 1 for axis in range(len(extent))])
    return factor_of


def scatter_about(own_key, extent, scale, reach, split=(), dtype=jnp.bfloat16):
    loudness = level_of(own_key, extent, split, -0.22, 0.18) if split else 1.0
    entries = jax.random.normal(own_key, extent, jnp.float32) * scale * loudness
    return jnp.minimum(jnp.maximum(entries, -reach), reach).astype(dtype)


def heavy_noise(rng, dims, width, most, pieces, heavy, held_as=jnp.bfloat16):
    array = width * jax.random.normal(rng, dims, jnp.float32)
    if pieces:
        array = array * level_of(rng, dims, pieces, -0.22, 0.18)
    return jnp.clip(raised(array, jax.random.fold_in(rng, 3), *heavy), -most, most).astype(held_as)


def setup_inputs(seed: int = 0) -> dict:
    arg_keys = jax.random.split(jax.random.key(seed), 7)
    return {
        "train_gate": heavy_noise(arg_keys[0], (EXPERTS, D_MODEL, D_EXPERT), D_MODEL ** -0.5, 0.25, ((0, 8), (1, 32)), (1, 2, 32, 2.75), jnp.float32),
        "other_gate": scatter_about(arg_keys[1], (EXPERTS, D_MODEL, D_EXPERT), (D_MODEL * 4) ** -0.5, 0.0625, ((0, 8), (1, 32))),
        "train_up": heavy_noise(arg_keys[2], (EXPERTS, D_MODEL, D_EXPERT), D_MODEL ** -0.5, 0.25, ((0, 8), (1, 32)), (1, 2, 32, 2.75), jnp.float32),
        "other_up": scatter_about(arg_keys[3], (EXPERTS, D_MODEL, D_EXPERT), (D_MODEL * 4) ** -0.5, 0.0625, ((0, 8), (1, 32))),
        "router_weight": scatter_about(arg_keys[4], (D_MODEL, EXPERTS), D_MODEL ** -0.5, 0.125, ((0, 32), (1, 8)), jnp.float32),
        "router_gain": jnp.clip(1.0 + 0.15 * jax.random.normal(arg_keys[5], (D_MODEL,), jnp.float32), 0.25, 1.75),
    }


def reference(train_gate, other_gate, train_up, other_up, router_weight, router_gain):
    latest_gate = train_gate + other_gate.astype(jnp.float32)
    latest_up = train_up + other_up.astype(jnp.float32)
    scale_gate = jnp.max(jnp.abs(latest_gate), axis=1)
    ready_gate = (latest_gate / jnp.expand_dims(scale_gate, 1)).astype(jnp.bfloat16)
    scale_up = jnp.max(jnp.abs(latest_up), axis=1)
    ready_up = (latest_up / jnp.expand_dims(scale_up, 1)).astype(jnp.bfloat16)
    serve_router = (router_weight * router_gain[:, None]).astype(jnp.bfloat16)
    return ready_gate, ready_up, scale_gate, scale_up, serve_router
```

```python
import functools

import jax
import jax.numpy as jnp
from jax import lax
from jax.experimental import pallas as pl
from jax.experimental.pallas import tpu as pltpu
from jax.sharding import PartitionSpec as P

MESH = pl.DeviceIdType.MESH
PER = 2


def kernel(
    n, nb, ny,
    tg, og, tu, ou, rw, rg,
    out_g, out_u, sc_out, router,
    tgv, ogv, tuv, ouv, part, gath, fin, scales, turned, send, recv, out_gv, out_uv, scv,
    rsend, rrecv, bsend, brecv, routerv,
    in_sem, part_send, part_recv, fin_send, fin_recv, main_send, main_recv,
    r_send, r_recv, b_send, b_recv, out_sem,
):
    experts, rows, cols = tgv.shape
    chunks = experts // PER
    wide = cols // n
    lanes = 2 * rows
    me = lax.axis_index("zero")
    bank = lax.axis_index("bank")
    nz = n // ny
    my_z, my_y = me // ny, me % ny

    def peer_of(k):
        step, dy = k // ny, k % ny
        dz = ((step % 2) * ((step + 1) // 2) + (1 - step % 2) * (nz - step // 2)) % nz
        return ((my_z + dz) % nz) * ny + (my_y + dy) % ny

    def load(c):
        at = pl.ds(c * PER, PER)
        return [
            pltpu.make_async_copy(src.at[at], dst.at[at], in_sem.at[i, c])
            for i, (src, dst) in enumerate(((tg, tgv), (og, ogv), (tu, tuv), (ou, ouv)))
        ]

    for c in range(chunks):
        for copy in load(c):
            copy.start()

    barrier = pltpu.get_barrier_semaphore()

    @pl.loop(1, n)
    def _(k):
        pl.semaphore_signal(barrier, inc=1, device_id={"zero": peer_of(k)}, device_id_type=MESH)

    @pl.loop(1, nb)
    def _(k):
        pl.semaphore_signal(barrier, inc=1, device_id={"bank": (bank + k) % nb}, device_id_type=MESH)

    block = rw[...] * rg[...]
    rsend[...] = jnp.concatenate([block, block], axis=1).astype(jnp.bfloat16)

    @pl.loop(0, chunks)
    def _(c):
        for copy in load(c):
            copy.wait()
        for j in range(PER):
            e = c * PER + j
            for kind, (t, o) in enumerate(((tgv, ogv), (tuv, ouv))):
                latest = t[e] + o[e].astype(jnp.float32)
                part[2 * e + kind] = jnp.max(jnp.abs(latest), axis=0, keepdims=True)

    pl.semaphore_wait(barrier, n - 1 + nb - 1)

    def send_part(row):
        return pltpu.make_async_remote_copy(
            src_ref=part.at[row], dst_ref=gath.at[me], send_sem=part_send, recv_sem=part_recv,
            device_id={"zero": row}, device_id_type=MESH,
        )

    @pl.loop(1, n)
    def _(k):
        send_part(peer_of(k)).start()

    gath[me] = part[me]

    @pl.loop(1, n)
    def _(k):
        pltpu.make_async_remote_copy(
            src_ref=rsend, dst_ref=rrecv.at[me], send_sem=r_send, recv_sem=r_recv,
            device_id={"zero": peer_of(k)}, device_id_type=MESH,
        ).start()

    rrecv[me] = rsend[...]

    pltpu.make_async_copy(gath.at[pl.ds(0, n - 1)], gath.at[pl.ds(0, n - 1)], part_recv).wait()
    total = gath[0]
    for k in range(1, n):
        total = jnp.maximum(total, gath[k])
    fin[0] = total
    scales[me] = total

    @pl.loop(1, n)
    def _(k):
        pltpu.make_async_remote_copy(
            src_ref=fin.at[0], dst_ref=scales.at[me], send_sem=fin_send, recv_sem=fin_recv.at[me],
            device_id={"zero": peer_of(k)}, device_id_type=MESH,
        ).start()

    @pl.loop(0, chunks)
    def _(c):
        for r in range(2 * PER):
            row = c * 2 * PER + r

            @pl.when(row != me)
            def _():
                pltpu.make_async_copy(scales.at[row], scales.at[row], fin_recv.at[row]).wait()

        for j in range(PER):
            e = c * PER + j
            inv_g = 1.0 / scales[2 * e]
            inv_u = 1.0 / scales[2 * e + 1]
            for b in range(cols // 128):
                at = slice(b * 128, (b + 1) * 128)
                gate = (tgv[e, :, at] + ogv[e, :, at].astype(jnp.float32)) * inv_g[:, at]
                up = (tuv[e, :, at] + ouv[e, :, at].astype(jnp.float32)) * inv_u[:, at]
                turned[j, at, :] = jnp.concatenate([gate, up], axis=0).T
        for p in range(n):
            both = jnp.concatenate([turned[j, p * wide : (p + 1) * wide, :] for j in range(PER)], axis=0)
            send[c, p] = both.astype(jnp.bfloat16)
        recv[c, me] = send[c, me]

        @pl.loop(1, n)
        def _(k):
            p = peer_of(k)
            pltpu.make_async_remote_copy(
                src_ref=send.at[c, p], dst_ref=recv.at[c, me], send_sem=main_send.at[c], recv_sem=main_recv.at[c],
                device_id={"zero": p}, device_id_type=MESH,
            ).start()

    pltpu.make_async_copy(rrecv.at[pl.ds(0, n - 1)], rrecv.at[pl.ds(0, n - 1)], r_recv).wait()
    low = lax.broadcasted_iota(jnp.int32, (experts, lanes), 1) < rows

    @pl.loop(0, n // 2)
    def _(k):
        pair = jnp.where(low, rrecv[2 * k].astype(jnp.float32), rrecv[2 * k + 1].astype(jnp.float32))
        bsend[k] = pair.astype(jnp.bfloat16)
        brecv[bank, k] = pair.astype(jnp.bfloat16)

    @pl.loop(1, nb)
    def _(k):
        pltpu.make_async_remote_copy(
            src_ref=bsend, dst_ref=brecv.at[bank], send_sem=b_send, recv_sem=b_recv,
            device_id={"bank": (bank + k) % nb}, device_id_type=MESH,
        ).start()

    table = jnp.concatenate([scales[r] for r in range(2 * experts)], axis=0)
    scv[...] = pltpu.roll(table, (cols - wide * me) % cols, 1)[:, :wide]
    sc_copy = pltpu.make_async_copy(scv, sc_out, out_sem.at[2, 0])
    sc_copy.start()

    pltpu.make_async_copy(brecv.at[pl.ds(0, nb - 1)], brecv.at[pl.ds(0, nb - 1)], b_recv).wait()

    @pl.loop(0, n // 2)
    def _(k):
        tall = jnp.concatenate([brecv[b, k].astype(jnp.float32) for b in range(nb)], axis=0)
        routerv[pl.ds(pl.multiple_of(k * lanes, lanes), lanes), :] = tall.T.astype(jnp.bfloat16)

    router_copy = pltpu.make_async_copy(routerv, router, out_sem.at[2, 1])
    router_copy.start()

    side = lax.broadcasted_iota(jnp.int32, (PER * wide, lanes), 1) < rows

    def store(c):
        at = pl.ds(c * PER, PER)
        return (
            pltpu.make_async_copy(out_gv.at[at], out_g.at[at], out_sem.at[0, c]),
            pltpu.make_async_copy(out_uv.at[at], out_u.at[at], out_sem.at[1, c]),
        )

    @pl.loop(0, chunks)
    def _(c):
        pltpu.make_async_copy(recv.at[c, pl.ds(0, n - 1)], recv.at[c, pl.ds(0, n - 1)], main_recv.at[c]).wait()
        for k in range(n // 2):
            a = recv[c, 2 * k].astype(jnp.float32)
            b = recv[c, 2 * k + 1].astype(jnp.float32)
            gate = jnp.where(side, a, pltpu.roll(b, rows, 1))
            up = jnp.where(side, pltpu.roll(a, rows, 1), b)
            for j in range(PER):
                part_rows = slice(j * wide, (j + 1) * wide)
                out_gv[c * PER + j, :, k * lanes : (k + 1) * lanes] = gate[part_rows].astype(jnp.bfloat16)
                out_uv[c * PER + j, :, k * lanes : (k + 1) * lanes] = up[part_rows].astype(jnp.bfloat16)
        for copy in store(c):
            copy.start()

    pltpu.make_async_copy(part.at[pl.ds(0, n - 1)], part.at[pl.ds(0, n - 1)], part_send).wait()
    pltpu.make_async_copy(scales.at[pl.ds(0, n - 1)], scales.at[pl.ds(0, n - 1)], fin_send).wait()
    pltpu.make_async_copy(rrecv.at[pl.ds(0, n - 1)], rrecv.at[pl.ds(0, n - 1)], r_send).wait()
    pltpu.make_async_copy(brecv.at[pl.ds(0, nb - 1)], brecv.at[pl.ds(0, nb - 1)], b_send).wait()
    for c in range(chunks):
        pltpu.make_async_copy(send.at[c, pl.ds(0, n - 1)], send.at[c, pl.ds(0, n - 1)], main_send.at[c]).wait()
        for copy in store(c):
            copy.wait()
    sc_copy.wait()
    router_copy.wait()


def solution(mesh):
    n, nb = mesh.shape["zero"], mesh.shape["bank"]
    ny = 4

    def on_device(train_gate, other_gate, train_up, other_up, router_weight, router_gain):
        experts, rows, cols = train_gate.shape
        wide, lanes, chunks = cols // n, 2 * rows, experts // PER
        f32, bf16 = jnp.float32, jnp.bfloat16
        hbm, vmem = pl.BlockSpec(memory_space=pl.ANY), pl.BlockSpec(memory_space=pltpu.VMEM)
        dma = pltpu.SemaphoreType.DMA
        out_g, out_u, sc, router = pl.pallas_call(
            functools.partial(kernel, n, nb, ny),
            out_shape=(
                jax.ShapeDtypeStruct((experts, wide, rows * n), bf16),
                jax.ShapeDtypeStruct((experts, wide, rows * n), bf16),
                jax.ShapeDtypeStruct((2 * experts, wide), f32),
                jax.ShapeDtypeStruct((rows * n, experts * nb), bf16),
            ),
            in_specs=[hbm] * 4 + [vmem] * 2,
            out_specs=(hbm,) * 4,
            scratch_shapes=[
                pltpu.VMEM((experts, rows, cols), f32),
                pltpu.VMEM((experts, rows, cols), bf16),
                pltpu.VMEM((experts, rows, cols), f32),
                pltpu.VMEM((experts, rows, cols), bf16),
                pltpu.VMEM((n, 1, cols), f32),
                pltpu.VMEM((n, 1, cols), f32),
                pltpu.VMEM((1, 1, cols), f32),
                pltpu.VMEM((n, 1, cols), f32),
                pltpu.VMEM((PER, cols, lanes), f32),
                pltpu.VMEM((chunks, n, PER * wide, lanes), bf16),
                pltpu.VMEM((chunks, n, PER * wide, lanes), bf16),
                pltpu.VMEM((experts, wide, rows * n), bf16),
                pltpu.VMEM((experts, wide, rows * n), bf16),
                pltpu.VMEM((2 * experts, wide), f32),
                pltpu.VMEM((experts, lanes), bf16),
                pltpu.VMEM((n, experts, lanes), bf16),
                pltpu.VMEM((n // 2, experts, lanes), bf16),
                pltpu.VMEM((nb, n // 2, experts, lanes), bf16),
                pltpu.VMEM((rows * n, experts * nb), bf16),
                dma((4, chunks)),
                dma, dma,
                dma, dma((n,)),
                dma((chunks,)), dma((chunks,)),
                dma, dma,
                dma, dma,
                dma((3, chunks)),
            ],
            compiler_params=pltpu.CompilerParams(
                collective_id=0, has_side_effects=True, vmem_limit_bytes=56 << 20
            ),
        )(train_gate, other_gate, train_up, other_up, router_weight.T, router_gain[None, :])
        scales = sc.reshape(experts, 2, wide)
        return (
            jnp.swapaxes(out_g, 1, 2),
            jnp.swapaxes(out_u, 1, 2),
            scales[:, 0],
            scales[:, 1],
            router,
        )

    return jax.shard_map(
        on_device,
        mesh=mesh,
        in_specs=(
            P("bank", "zero", None),
            P("bank", "zero", None),
            P("bank", "zero", None),
            P("bank", "zero", None),
            P("zero", "bank"),
            P("zero"),
        ),
        out_specs=(
            P("bank", None, "zero"),
            P("bank", None, "zero"),
            P("bank", "zero"),
            P("bank", "zero"),
            P(),
        ),
        check_vma=False,
    )
```

```python
import functools

import jax
import jax.numpy as jnp
from jax import lax
from jax.experimental import pallas as pl
from jax.experimental.pallas import tpu as pltpu
from jax.sharding import PartitionSpec as P

MESH = pl.DeviceIdType.MESH
PER = 1


def kernel(
    n, nb,
    tg, og, tu, ou, rw, rg,
    out_gv, out_uv, sc_g, sc_u, routerv,
    tgv, ogv, tuv, ouv, rwv, rgv, part, gath, fin, scales, turned, send, recv,
    rsend, rrecv, bsend, brecv,
    in_sem, rw_sem, part_send, part_recv, fin_send, fin_recv, main_send, main_recv,
    r_send, r_recv, b_send, b_recv,
):
    experts, rows, cols = tgv.shape
    chunks = experts // PER
    wide = cols // n
    lanes = 2 * rows
    me = lax.axis_index("zero")
    bank = lax.axis_index("bank")

    def peer_of(k):
        p = me + k
        return jnp.where(p >= n, p - n, p)

    def mate_of(k):
        p = bank + k
        return jnp.where(p >= nb, p - nb, p)

    offsets = sorted(range(1, n), key=lambda k: -min(k, n - k))
    strides = sorted(range(1, nb), key=lambda k: -min(k, nb - k))

    def load(c):
        at = pl.ds(c * PER, PER)
        return [
            pltpu.make_async_copy(src.at[at], dst.at[at], in_sem.at[i, c])
            for i, (src, dst) in enumerate(((tg, tgv), (og, ogv), (tu, tuv), (ou, ouv)))
        ]

    barrier = pltpu.get_barrier_semaphore()

    for k in offsets:
        pl.semaphore_signal(barrier, inc=1, device_id={"zero": peer_of(k)}, device_id_type=MESH)

    for k in strides:
        pl.semaphore_signal(barrier, inc=1, device_id={"bank": mate_of(k)}, device_id_type=MESH)

    for c in range(chunks):
        for copy in load(c):
            copy.start()

    rw_loads = (pltpu.make_async_copy(rw, rwv, rw_sem.at[0]), pltpu.make_async_copy(rg, rgv, rw_sem.at[1]))
    for copy in rw_loads:
        copy.start()

    def send_part(row):
        return pltpu.make_async_remote_copy(
            src_ref=part.at[row], dst_ref=gath.at[me], send_sem=part_send, recv_sem=part_recv,
            device_id={"zero": row}, device_id_type=MESH,
        )

    def largest(c):
        for copy in load(c):
            copy.wait()
        for j in range(PER):
            e = c * PER + j
            for kind, (t, o) in enumerate(((tgv, ogv), (tuv, ouv))):
                latest = t[e] + o[e].astype(jnp.float32)
                part[2 * e + kind] = jnp.max(jnp.abs(latest), axis=0, keepdims=True)

    def pass_on(c):
        for r in range(2 * PER):
            row = c * 2 * PER + r

            @pl.when(row != me)
            def _():
                send_part(row).start()

    largest(0)
    pl.semaphore_wait(barrier, n - 1 + nb - 1)
    pass_on(0)

    @pl.loop(1, chunks)
    def _(c):
        largest(c)
        pass_on(c)

    gath[me] = part[me]

    for copy in rw_loads:
        copy.wait()
    block = rwv[...] * rgv[...]
    rsend[...] = jnp.concatenate([block, block], axis=1).astype(jnp.bfloat16)

    for k in offsets:
        pltpu.make_async_remote_copy(
            src_ref=rsend, dst_ref=rrecv.at[me], send_sem=r_send, recv_sem=r_recv,
            device_id={"zero": peer_of(k)}, device_id_type=MESH,
        ).start()

    rrecv[me] = rsend[...]

    pltpu.make_async_copy(gath.at[pl.ds(0, n - 1)], gath.at[pl.ds(0, n - 1)], part_recv).wait()
    total = gath[0]
    for k in range(1, n):
        total = jnp.maximum(total, gath[k])
    fin[0] = total
    scales[me] = total

    for k in offsets:
        pltpu.make_async_remote_copy(
            src_ref=fin.at[0], dst_ref=scales.at[me], send_sem=fin_send, recv_sem=fin_recv.at[me],
            device_id={"zero": peer_of(k)}, device_id_type=MESH,
        ).start()

    @pl.loop(0, chunks)
    def _(c):
        for r in range(2 * PER):
            row = c * 2 * PER + r

            @pl.when(row != me)
            def _():
                pltpu.make_async_copy(scales.at[row], scales.at[row], fin_recv.at[row]).wait()

        for j in range(PER):
            e = c * PER + j
            inv_g = 1.0 / scales[2 * e]
            inv_u = 1.0 / scales[2 * e + 1]
            for b in range(cols // 128):
                at = slice(b * 128, (b + 1) * 128)
                gate = (tgv[e, :, at] + ogv[e, :, at].astype(jnp.float32)) * inv_g[:, at]
                up = (tuv[e, :, at] + ouv[e, :, at].astype(jnp.float32)) * inv_u[:, at]
                turned[j, at, :] = jnp.concatenate([gate, up], axis=0).T
        for p in range(n):
            both = jnp.concatenate([turned[j, p * wide : (p + 1) * wide, :] for j in range(PER)], axis=0)
            send[c, p] = both.astype(jnp.bfloat16)
        recv[c, me] = send[c, me]

        for k in offsets:
            p = peer_of(k)
            pltpu.make_async_remote_copy(
                src_ref=send.at[c, p], dst_ref=recv.at[c, me], send_sem=main_send.at[c], recv_sem=main_recv.at[c],
                device_id={"zero": p}, device_id_type=MESH,
            ).start()

    pltpu.make_async_copy(rrecv.at[pl.ds(0, n - 1)], rrecv.at[pl.ds(0, n - 1)], r_recv).wait()
    low = lax.broadcasted_iota(jnp.int32, (experts, lanes), 1) < rows

    @pl.loop(0, n // 2)
    def _(k):
        pair = jnp.where(low, rrecv[2 * k].astype(jnp.float32), rrecv[2 * k + 1].astype(jnp.float32))
        bsend[k] = pair.astype(jnp.bfloat16)
        brecv[bank, k] = pair.astype(jnp.bfloat16)

    for k in strides:
        pltpu.make_async_remote_copy(
            src_ref=bsend, dst_ref=brecv.at[bank], send_sem=b_send, recv_sem=b_recv,
            device_id={"bank": mate_of(k)}, device_id_type=MESH,
        ).start()

    for scv, kind in ((sc_g, 0), (sc_u, 1)):
        table = jnp.concatenate([scales[2 * e + kind] for e in range(experts)], axis=0)
        scv[...] = pltpu.roll(table, (cols - wide * me) % cols, 1)[:, :wide]

    pltpu.make_async_copy(brecv.at[pl.ds(0, nb - 1)], brecv.at[pl.ds(0, nb - 1)], b_recv).wait()

    @pl.loop(0, n // 2)
    def _(k):
        tall = jnp.concatenate([brecv[b, k].astype(jnp.float32) for b in range(nb)], axis=0)
        routerv[pl.ds(pl.multiple_of(k * lanes, lanes), lanes), :] = tall.T.astype(jnp.bfloat16)

    side = lax.broadcasted_iota(jnp.int32, (PER * wide, lanes), 1) < rows

    @pl.loop(0, chunks)
    def _(c):
        pltpu.make_async_copy(recv.at[c, pl.ds(0, n - 1)], recv.at[c, pl.ds(0, n - 1)], main_recv.at[c]).wait()
        for k in range(n // 2):
            a = recv[c, 2 * k].astype(jnp.float32)
            b = recv[c, 2 * k + 1].astype(jnp.float32)
            gate = jnp.where(side, a, pltpu.roll(b, rows, 1))
            up = jnp.where(side, pltpu.roll(a, rows, 1), b)
            for j in range(PER):
                part_rows = slice(j * wide, (j + 1) * wide)
                out_gv[c * PER + j, :, k * lanes : (k + 1) * lanes] = gate[part_rows].astype(jnp.bfloat16)
                out_uv[c * PER + j, :, k * lanes : (k + 1) * lanes] = up[part_rows].astype(jnp.bfloat16)

    pltpu.make_async_copy(part.at[pl.ds(0, n - 1)], part.at[pl.ds(0, n - 1)], part_send).wait()
    pltpu.make_async_copy(scales.at[pl.ds(0, n - 1)], scales.at[pl.ds(0, n - 1)], fin_send).wait()
    pltpu.make_async_copy(rrecv.at[pl.ds(0, n - 1)], rrecv.at[pl.ds(0, n - 1)], r_send).wait()
    pltpu.make_async_copy(brecv.at[pl.ds(0, nb - 1)], brecv.at[pl.ds(0, nb - 1)], b_send).wait()
    for c in range(chunks):
        pltpu.make_async_copy(send.at[c, pl.ds(0, n - 1)], send.at[c, pl.ds(0, n - 1)], main_send.at[c]).wait()


def store(*refs):
    arrays = len(refs) // 2
    ins, outs, sem = refs[:arrays], refs[arrays : 2 * arrays], refs[-1]
    copies = [pltpu.make_async_copy(i, o, sem.at[k]) for k, (i, o) in enumerate(zip(ins, outs))]
    for copy in copies:
        copy.start()
    for copy in copies:
        copy.wait()


def solution(mesh):
    n, nb = mesh.shape["zero"], mesh.shape["bank"]

    def on_device(train_gate, other_gate, train_up, other_up, router_weight, router_gain):
        experts, rows, cols = train_gate.shape
        wide, lanes, chunks = cols // n, 2 * rows, experts // PER
        f32, bf16 = jnp.float32, jnp.bfloat16
        hbm, vmem = pl.BlockSpec(memory_space=pltpu.HBM), pl.BlockSpec(memory_space=pltpu.VMEM)
        dma = pltpu.SemaphoreType.DMA
        shapes = (
            jax.ShapeDtypeStruct((experts, wide, rows * n), bf16),
            jax.ShapeDtypeStruct((experts, wide, rows * n), bf16),
            jax.ShapeDtypeStruct((experts, wide), f32),
            jax.ShapeDtypeStruct((experts, wide), f32),
            jax.ShapeDtypeStruct((rows * n, experts * nb), bf16),
        )
        held = pl.pallas_call(
            functools.partial(kernel, n, nb),
            out_shape=tuple(pltpu.VMEM(a.shape, a.dtype) for a in shapes),
            in_specs=[hbm] * 6,
            out_specs=(vmem,) * 5,
            scratch_shapes=[
                pltpu.VMEM((experts, rows, cols), f32),
                pltpu.VMEM((experts, rows, cols), bf16),
                pltpu.VMEM((experts, rows, cols), f32),
                pltpu.VMEM((experts, rows, cols), bf16),
                pltpu.VMEM((experts, rows), f32),
                pltpu.VMEM((1, rows), f32),
                pltpu.VMEM((n, 1, cols), f32),
                pltpu.VMEM((n, 1, cols), f32),
                pltpu.VMEM((1, 1, cols), f32),
                pltpu.VMEM((n, 1, cols), f32),
                pltpu.VMEM((PER, cols, lanes), f32),
                pltpu.VMEM((chunks, n, PER * wide, lanes), bf16),
                pltpu.VMEM((chunks, n, PER * wide, lanes), bf16),
                pltpu.VMEM((experts, lanes), bf16),
                pltpu.VMEM((n, experts, lanes), bf16),
                pltpu.VMEM((n // 2, experts, lanes), bf16),
                pltpu.VMEM((nb, n // 2, experts, lanes), bf16),
                dma((4, chunks)),
                dma((2,)),
                dma, dma,
                dma, dma((n,)),
                dma((chunks,)), dma((chunks,)),
                dma, dma,
                dma, dma,
            ],
            compiler_params=pltpu.CompilerParams(
                collective_id=0, has_side_effects=True, vmem_limit_bytes=40 << 20
            ),
        )(
            *(
                pltpu.with_memory_space_constraint(a, pltpu.HBM)
                for a in (train_gate, other_gate, train_up, other_up, router_weight.T, router_gain[None, :])
            )
        )
        out_g, out_u, sc_g, sc_u, router = pl.pallas_call(
            store,
            out_shape=shapes,
            in_specs=[vmem] * 5,
            out_specs=(hbm,) * 5,
            scratch_shapes=[dma((5,))],
            compiler_params=pltpu.CompilerParams(vmem_limit_bytes=4 << 20),
        )(*held)
        return jnp.swapaxes(out_g, 1, 2), jnp.swapaxes(out_u, 1, 2), sc_g, sc_u, router

    return jax.shard_map(
        on_device,
        mesh=mesh,
        in_specs=(
            P("bank", "zero", None),
            P("bank", "zero", None),
            P("bank", "zero", None),
            P("bank", "zero", None),
            P("zero", "bank"),
            P("zero"),
        ),
        out_specs=(
            P("bank", None, "zero"),
            P("bank", None, "zero"),
            P("bank", "zero"),
            P("bank", "zero"),
            P(),
        ),
        check_vma=False,
    )
```

```python
import functools

import jax
import jax.numpy as jnp
from jax import lax
from jax.experimental import pallas as pl
from jax.experimental.pallas import tpu as pltpu
from jax.sharding import PartitionSpec as P

MESH = pl.DeviceIdType.MESH
PER = 1


def kernel(
    n, nb,
    tg, og, tu, ou, rw, rg,
    out_gv, out_uv, sc_g, sc_u, routerv,
    tgv, ogv, tuv, ouv, rwv, rgv, part, gath, fin, scales, turned, send, recv,
    rsend, rrecv, bsend, brecv,
    in_sem, rw_sem, part_send, part_recv, fin_send, fin_recv, main_send, main_recv,
    r_send, r_recv, b_send, b_recv,
):
    experts, rows, cols = tgv.shape
    chunks = experts // PER
    wide = cols // n
    lanes = 2 * rows
    half = experts // 2
    me = lax.axis_index("zero")
    bank = lax.axis_index("bank")

    def peer_of(k):
        p = me + k
        return jnp.where(p >= n, p - n, p)

    def mate_of(k):
        p = bank + k
        return jnp.where(p >= nb, p - nb, p)

    offsets = sorted(range(1, n), key=lambda k: -min(k, n - k))
    strides = sorted(range(1, nb), key=lambda k: -min(k, nb - k))

    def load(c):
        at = pl.ds(c * PER, PER)
        return [
            pltpu.make_async_copy(src.at[at], dst.at[at], in_sem.at[i, c])
            for i, (src, dst) in enumerate(((tg, tgv), (og, ogv), (tu, tuv), (ou, ouv)))
        ]

    barrier = pltpu.get_barrier_semaphore()

    for k in offsets:
        pl.semaphore_signal(barrier, inc=1, device_id={"zero": peer_of(k)}, device_id_type=MESH)

    for k in strides:
        pl.semaphore_signal(barrier, inc=1, device_id={"bank": mate_of(k)}, device_id_type=MESH)

    for c in range(chunks):
        for copy in load(c):
            copy.start()

    rw_loads = (pltpu.make_async_copy(rw, rwv, rw_sem.at[0]), pltpu.make_async_copy(rg, rgv, rw_sem.at[1]))
    for copy in rw_loads:
        copy.start()

    def send_part(row):
        return pltpu.make_async_remote_copy(
            src_ref=part.at[row], dst_ref=gath.at[me], send_sem=part_send, recv_sem=part_recv,
            device_id={"zero": row}, device_id_type=MESH,
        )

    def largest(c):
        for copy in load(c):
            copy.wait()
        for j in range(PER):
            e = c * PER + j
            for kind, (t, o) in enumerate(((tgv, ogv), (tuv, ouv))):
                latest = t[e] + o[e].astype(jnp.float32)
                part[2 * e + kind] = jnp.max(jnp.abs(latest), axis=0, keepdims=True)

    def pass_on(c):
        for r in range(2 * PER):
            row = c * 2 * PER + r

            @pl.when(row != me)
            def _():
                send_part(row).start()

    largest(0)
    pl.semaphore_wait(barrier, n - 1 + nb - 1)
    pass_on(0)

    @pl.loop(1, chunks)
    def _(c):
        largest(c)
        pass_on(c)

    gath[me] = part[me]

    for copy in rw_loads:
        copy.wait()
    block = rwv[...] * rgv[...]
    rsend[...] = jnp.concatenate([block[:half], block[half:]], axis=1).astype(jnp.bfloat16)

    for k in offsets:
        pltpu.make_async_remote_copy(
            src_ref=rsend, dst_ref=rrecv.at[me], send_sem=r_send, recv_sem=r_recv,
            device_id={"zero": peer_of(k)}, device_id_type=MESH,
        ).start()

    rrecv[me] = rsend[...]

    pltpu.make_async_copy(gath.at[pl.ds(0, n - 1)], gath.at[pl.ds(0, n - 1)], part_recv).wait()
    total = gath[0]
    for k in range(1, n):
        total = jnp.maximum(total, gath[k])
    fin[0] = total
    scales[me] = total

    for k in offsets:
        pltpu.make_async_remote_copy(
            src_ref=fin.at[0], dst_ref=scales.at[me], send_sem=fin_send, recv_sem=fin_recv.at[me],
            device_id={"zero": peer_of(k)}, device_id_type=MESH,
        ).start()

    @pl.loop(0, chunks)
    def _(c):
        for r in range(2 * PER):
            row = c * 2 * PER + r

            @pl.when(row != me)
            def _():
                pltpu.make_async_copy(scales.at[row], scales.at[row], fin_recv.at[row]).wait()

        for j in range(PER):
            e = c * PER + j
            inv_g = 1.0 / scales[2 * e]
            inv_u = 1.0 / scales[2 * e + 1]
            for b in range(cols // 128):
                at = slice(b * 128, (b + 1) * 128)
                gate = (tgv[e, :, at] + ogv[e, :, at].astype(jnp.float32)) * inv_g[:, at]
                up = (tuv[e, :, at] + ouv[e, :, at].astype(jnp.float32)) * inv_u[:, at]
                turned[j, at, :] = jnp.concatenate([gate, up], axis=0).T
        for p in range(n):
            both = jnp.concatenate([turned[j, p * wide : (p + 1) * wide, :] for j in range(PER)], axis=0)
            send[c, p] = both.astype(jnp.bfloat16)
        recv[c, me] = send[c, me]

        for k in offsets:
            p = peer_of(k)
            pltpu.make_async_remote_copy(
                src_ref=send.at[c, p], dst_ref=recv.at[c, me], send_sem=main_send.at[c], recv_sem=main_recv.at[c],
                device_id={"zero": p}, device_id_type=MESH,
            ).start()

    pltpu.make_async_copy(rrecv.at[pl.ds(0, n - 1)], rrecv.at[pl.ds(0, n - 1)], r_recv).wait()
    low = lax.broadcasted_iota(jnp.int32, (half, lanes), 1) < rows

    @pl.loop(0, n // 2)
    def _(k):
        a = rrecv[2 * k].astype(jnp.float32)
        b = rrecv[2 * k + 1].astype(jnp.float32)
        first = jnp.where(low, a, pltpu.roll(b, rows, 1))
        second = jnp.where(low, pltpu.roll(a, rows, 1), b)
        pair = jnp.concatenate([first, second], axis=0).astype(jnp.bfloat16)
        bsend[k] = pair
        brecv[bank, k] = pair

    for k in strides:
        pltpu.make_async_remote_copy(
            src_ref=bsend, dst_ref=brecv.at[bank], send_sem=b_send, recv_sem=b_recv,
            device_id={"bank": mate_of(k)}, device_id_type=MESH,
        ).start()

    for scv, kind in ((sc_g, 0), (sc_u, 1)):
        table = jnp.concatenate([scales[2 * e + kind] for e in range(experts)], axis=0)
        scv[...] = pltpu.roll(table, (cols - wide * me) % cols, 1)[:, :wide]

    pltpu.make_async_copy(brecv.at[pl.ds(0, nb - 1)], brecv.at[pl.ds(0, nb - 1)], b_recv).wait()

    @pl.loop(0, n // 2)
    def _(k):
        tall = jnp.concatenate([brecv[b, k].astype(jnp.float32) for b in range(nb)], axis=0)
        routerv[pl.ds(pl.multiple_of(k * lanes, lanes), lanes), :] = tall.T.astype(jnp.bfloat16)

    side = lax.broadcasted_iota(jnp.int32, (PER * wide, lanes), 1) < rows

    @pl.loop(0, chunks)
    def _(c):
        pltpu.make_async_copy(recv.at[c, pl.ds(0, n - 1)], recv.at[c, pl.ds(0, n - 1)], main_recv.at[c]).wait()
        for k in range(n // 2):
            a = recv[c, 2 * k].astype(jnp.float32)
            b = recv[c, 2 * k + 1].astype(jnp.float32)
            gate = jnp.where(side, a, pltpu.roll(b, rows, 1))
            up = jnp.where(side, pltpu.roll(a, rows, 1), b)
            for j in range(PER):
                part_rows = slice(j * wide, (j + 1) * wide)
                out_gv[c * PER + j, :, k * lanes : (k + 1) * lanes] = gate[part_rows].astype(jnp.bfloat16)
                out_uv[c * PER + j, :, k * lanes : (k + 1) * lanes] = up[part_rows].astype(jnp.bfloat16)

    pltpu.make_async_copy(part.at[pl.ds(0, n - 1)], part.at[pl.ds(0, n - 1)], part_send).wait()
    pltpu.make_async_copy(scales.at[pl.ds(0, n - 1)], scales.at[pl.ds(0, n - 1)], fin_send).wait()
    pltpu.make_async_copy(rrecv.at[pl.ds(0, n - 1)], rrecv.at[pl.ds(0, n - 1)], r_send).wait()
    pltpu.make_async_copy(brecv.at[pl.ds(0, nb - 1)], brecv.at[pl.ds(0, nb - 1)], b_send).wait()
    for c in range(chunks):
        pltpu.make_async_copy(send.at[c, pl.ds(0, n - 1)], send.at[c, pl.ds(0, n - 1)], main_send.at[c]).wait()


def store(*refs):
    arrays = len(refs) // 2
    ins, outs, sem = refs[:arrays], refs[arrays : 2 * arrays], refs[-1]
    copies = [pltpu.make_async_copy(i, o, sem.at[k]) for k, (i, o) in enumerate(zip(ins, outs))]
    for copy in copies:
        copy.start()
    for copy in copies:
        copy.wait()


def solution(mesh):
    n, nb = mesh.shape["zero"], mesh.shape["bank"]

    def on_device(train_gate, other_gate, train_up, other_up, router_weight, router_gain):
        experts, rows, cols = train_gate.shape
        wide, lanes, chunks = cols // n, 2 * rows, experts // PER
        f32, bf16 = jnp.float32, jnp.bfloat16
        hbm, vmem = pl.BlockSpec(memory_space=pltpu.HBM), pl.BlockSpec(memory_space=pltpu.VMEM)
        dma = pltpu.SemaphoreType.DMA
        shapes = (
            jax.ShapeDtypeStruct((experts, wide, rows * n), bf16),
            jax.ShapeDtypeStruct((experts, wide, rows * n), bf16),
            jax.ShapeDtypeStruct((experts, wide), f32),
            jax.ShapeDtypeStruct((experts, wide), f32),
            jax.ShapeDtypeStruct((rows * n, experts * nb), bf16),
        )
        held = pl.pallas_call(
            functools.partial(kernel, n, nb),
            out_shape=tuple(pltpu.VMEM(a.shape, a.dtype) for a in shapes),
            in_specs=[hbm] * 6,
            out_specs=(vmem,) * 5,
            scratch_shapes=[
                pltpu.VMEM((experts, rows, cols), f32),
                pltpu.VMEM((experts, rows, cols), bf16),
                pltpu.VMEM((experts, rows, cols), f32),
                pltpu.VMEM((experts, rows, cols), bf16),
                pltpu.VMEM((experts, rows), f32),
                pltpu.VMEM((1, rows), f32),
                pltpu.VMEM((n, 1, cols), f32),
                pltpu.VMEM((n, 1, cols), f32),
                pltpu.VMEM((1, 1, cols), f32),
                pltpu.VMEM((n, 1, cols), f32),
                pltpu.VMEM((PER, cols, lanes), f32),
                pltpu.VMEM((chunks, n, PER * wide, lanes), bf16),
                pltpu.VMEM((chunks, n, PER * wide, lanes), bf16),
                pltpu.VMEM((experts // 2, lanes), bf16),
                pltpu.VMEM((n, experts // 2, lanes), bf16),
                pltpu.VMEM((n // 2, experts, lanes), bf16),
                pltpu.VMEM((nb, n // 2, experts, lanes), bf16),
                dma((4, chunks)),
                dma((2,)),
                dma, dma,
                dma, dma((n,)),
                dma((chunks,)), dma((chunks,)),
                dma, dma,
                dma, dma,
            ],
            compiler_params=pltpu.CompilerParams(
                collective_id=0, has_side_effects=True, vmem_limit_bytes=40 << 20
            ),
        )(
            *(
                pltpu.with_memory_space_constraint(a, pltpu.HBM)
                for a in (train_gate, other_gate, train_up, other_up, router_weight.T, router_gain[None, :])
            )
        )
        out_g, out_u, sc_g, sc_u, router = pl.pallas_call(
            store,
            out_shape=shapes,
            in_specs=[vmem] * 5,
            out_specs=(hbm,) * 5,
            scratch_shapes=[dma((5,))],
            compiler_params=pltpu.CompilerParams(vmem_limit_bytes=4 << 20),
        )(*held)
        return jnp.swapaxes(out_g, 1, 2), jnp.swapaxes(out_u, 1, 2), sc_g, sc_u, router

    return jax.shard_map(
        on_device,
        mesh=mesh,
        in_specs=(
            P("bank", "zero", None),
            P("bank", "zero", None),
            P("bank", "zero", None),
            P("bank", "zero", None),
            P("zero", "bank"),
            P("zero"),
        ),
        out_specs=(
            P("bank", None, "zero"),
            P("bank", None, "zero"),
            P("bank", "zero"),
            P("bank", "zero"),
            P(),
        ),
        check_vma=False,
    )
```

```python
import functools

import jax
import jax.numpy as jnp
from jax import lax
from jax.experimental import pallas as pl
from jax.experimental.pallas import tpu as pltpu
from jax.sharding import PartitionSpec as P

MESH = pl.DeviceIdType.MESH
NY = 4


def kernel(
    n, nb,
    tg, og, tu, ou, rw, rg,
    out_gv, out_uv, sc_g, sc_u, routerv,
    tgv, ogv, tuv, ouv, rwv, rgv, part, gath, fin, scales, turned, send, recv,
    rsend, rrecv, bsend, brecv,
    in_sem, rw_sem, part_send, part_recv, fin_send, fin_recv, side_send, side_recv, main_send, main_recv,
    r_send, r_recv, b_send, b_recv,
):
    experts, rows, cols = tgv.shape
    chunks = experts
    wide = cols // n
    lanes = 2 * rows
    half = experts // 2
    me = lax.axis_index("zero")
    bank = lax.axis_index("bank")

    def mate_of(k):
        p = bank + k
        return jnp.where(p >= nb, p - nb, p)

    my_z = lax.div(me, NY)
    my_y = me - my_z * NY
    nz = n // NY

    def peer_of(k):
        z, y = my_z + k // NY, my_y + k % NY
        return jnp.where(z >= nz, z - nz, z) * NY + jnp.where(y >= NY, y - NY, y)

    def place(r):
        return r % NY * nz + r // NY

    def hops(k):
        return min(k // NY, nz - k // NY), min(k % NY, NY - k % NY)

    offsets = sorted(range(1, n), key=lambda k: (-hops(k)[0], -hops(k)[1]))
    strides = sorted(range(1, nb), key=lambda k: -min(k, nb - k))

    def load(c):
        at = pl.ds(c, 1)
        return [
            pltpu.make_async_copy(src.at[at], dst.at[at], in_sem.at[i, c])
            for i, (src, dst) in enumerate(((tg, tgv), (og, ogv), (tu, tuv), (ou, ouv)))
        ]

    for copy in load(0):
        copy.start()

    barrier = pltpu.get_barrier_semaphore()

    for k in offsets:
        pl.semaphore_signal(barrier, inc=1, device_id={"zero": peer_of(k)}, device_id_type=MESH)

    for k in strides:
        pl.semaphore_signal(barrier, inc=1, device_id={"bank": mate_of(k)}, device_id_type=MESH)

    for c in range(1, chunks):
        for copy in load(c):
            copy.start()

    rw_loads = (pltpu.make_async_copy(rw, rwv, rw_sem.at[0]), pltpu.make_async_copy(rg, rgv, rw_sem.at[1]))
    for copy in rw_loads:
        copy.start()

    def send_part(row):
        return pltpu.make_async_remote_copy(
            src_ref=part.at[row], dst_ref=gath.at[me], send_sem=part_send, recv_sem=part_recv,
            device_id={"zero": row}, device_id_type=MESH,
        )

    def largest(c):
        for copy in load(c):
            copy.wait()
        for kind, (t, o) in enumerate(((tgv, ogv), (tuv, ouv))):
            latest = t[c] + o[c].astype(jnp.float32)
            part[2 * c + kind] = jnp.max(jnp.abs(latest), axis=0, keepdims=True)

    def pass_on(c):
        for row in (2 * c, 2 * c + 1):

            @pl.when(row != me)
            def _():
                send_part(row).start()

    largest(0)
    pl.semaphore_wait(barrier, n - 1 + nb - 1)
    pass_on(0)

    @pl.loop(1, chunks)
    def _(c):
        largest(c)
        pass_on(c)

    gath[me] = part[me]

    for copy in rw_loads:
        copy.wait()
    block = rwv[...] * rgv[...]
    rsend[...] = jnp.concatenate([block[:half], block[half:]], axis=1).astype(jnp.bfloat16)

    for k in offsets:
        pltpu.make_async_remote_copy(
            src_ref=rsend, dst_ref=rrecv.at[me], send_sem=r_send, recv_sem=r_recv,
            device_id={"zero": peer_of(k)}, device_id_type=MESH,
        ).start()

    rrecv[me] = rsend[...]

    pltpu.make_async_copy(gath.at[pl.ds(0, n - 1)], gath.at[pl.ds(0, n - 1)], part_recv).wait()
    total = gath[0]
    for k in range(1, n):
        total = jnp.maximum(total, gath[k])
    fin[0] = total
    scales[my_y * nz + my_z] = total

    def send_fin(peer):
        return pltpu.make_async_remote_copy(
            src_ref=fin.at[0], dst_ref=scales.at[my_y * nz + my_z], send_sem=fin_send, recv_sem=fin_recv.at[me],
            device_id={"zero": peer}, device_id_type=MESH,
        )

    @pl.when(my_z == 0)
    def _():
        for k in offsets:
            send_fin(peer_of(k)).start()

    @pl.when(my_z > 0)
    def _():
        for k in sorted(range(1, nz), key=lambda k: -min(k, nz - k)):
            send_fin(peer_of(k * NY)).start()

    def take_fin(row, at):
        pltpu.make_async_copy(scales.at[at], scales.at[at], fin_recv.at[row]).wait()

    for r in range(NY):

        @pl.when(me != r)
        def _():
            take_fin(r, place(r))

    def post(c):
        y, z = lax.rem(2 * c, NY), lax.div(2 * c, NY)
        inv_g = 1.0 / scales[y * nz + z]
        inv_u = 1.0 / scales[(y + 1) * nz + z]
        for b in range(cols // 128):
            at = slice(b * 128, (b + 1) * 128)
            gate = (tgv[c, :, at] + ogv[c, :, at].astype(jnp.float32)) * inv_g[:, at]
            up = (tuv[c, :, at] + ouv[c, :, at].astype(jnp.float32)) * inv_u[:, at]
            turned[at, :] = jnp.concatenate([gate, up], axis=0).T
        for p in range(n):
            send[c, p] = turned[p * wide : (p + 1) * wide, :].astype(jnp.bfloat16)
        recv[c, me] = send[c, me]
        for k in offsets:
            p = peer_of(k)
            pltpu.make_async_remote_copy(
                src_ref=send.at[c, p], dst_ref=recv.at[c, me], send_sem=main_send.at[c], recv_sem=main_recv.at[c],
                device_id={"zero": p}, device_id_type=MESH,
            ).start()

    def send_rows(k):
        at = pl.ds(my_y * nz + 1, nz - 1)
        return pltpu.make_async_remote_copy(
            src_ref=scales.at[at], dst_ref=scales.at[at], send_sem=side_send, recv_sem=side_recv.at[my_y],
            device_id={"zero": peer_of(k)}, device_id_type=MESH,
        )

    post(0)
    for z in range(1, nz):

        @pl.when(my_z != z)
        def _():
            take_fin(z * NY + my_y, my_y * nz + z)

    for k in range(1, NY):
        send_rows(k).start()
    post(1)
    for y in range(NY):

        @pl.when(my_y != y)
        def _():
            at = pl.ds(y * nz + 1, nz - 1)
            pltpu.make_async_copy(scales.at[at], scales.at[at], side_recv.at[y]).wait()

    pl.loop(2, chunks)(post)

    pltpu.make_async_copy(rrecv.at[pl.ds(0, n - 1)], rrecv.at[pl.ds(0, n - 1)], r_recv).wait()
    low = lax.broadcasted_iota(jnp.int32, (half, lanes), 1) < rows

    @pl.loop(0, n // 2)
    def _(k):
        a = rrecv[2 * k].astype(jnp.float32)
        b = rrecv[2 * k + 1].astype(jnp.float32)
        first = jnp.where(low, a, pltpu.roll(b, rows, 1))
        second = jnp.where(low, pltpu.roll(a, rows, 1), b)
        pair = jnp.concatenate([first, second], axis=0).astype(jnp.bfloat16)
        bsend[k] = pair
        brecv[bank, k] = pair

    for k in strides:
        pltpu.make_async_remote_copy(
            src_ref=bsend, dst_ref=brecv.at[bank], send_sem=b_send, recv_sem=b_recv,
            device_id={"bank": mate_of(k)}, device_id_type=MESH,
        ).start()

    for scv, kind in ((sc_g, 0), (sc_u, 1)):
        table = jnp.concatenate([scales[place(2 * e + kind)] for e in range(experts)], axis=0)
        scv[...] = pltpu.roll(table, (cols - wide * me) % cols, 1)[:, :wide]

    pltpu.make_async_copy(brecv.at[pl.ds(0, nb - 1)], brecv.at[pl.ds(0, nb - 1)], b_recv).wait()

    @pl.loop(0, n // 2)
    def _(k):
        tall = jnp.concatenate([brecv[b, k].astype(jnp.float32) for b in range(nb)], axis=0)
        routerv[pl.ds(pl.multiple_of(k * lanes, lanes), lanes), :] = tall.T.astype(jnp.bfloat16)

    side = lax.broadcasted_iota(jnp.int32, (wide, lanes), 1) < rows

    @pl.loop(0, chunks)
    def _(c):
        pltpu.make_async_copy(recv.at[c, pl.ds(0, n - 1)], recv.at[c, pl.ds(0, n - 1)], main_recv.at[c]).wait()
        for k in range(n // 2):
            a = recv[c, 2 * k].astype(jnp.float32)
            b = recv[c, 2 * k + 1].astype(jnp.float32)
            gate = jnp.where(side, a, pltpu.roll(b, rows, 1))
            up = jnp.where(side, pltpu.roll(a, rows, 1), b)
            out_gv[c, :, k * lanes : (k + 1) * lanes] = gate.astype(jnp.bfloat16)
            out_uv[c, :, k * lanes : (k + 1) * lanes] = up.astype(jnp.bfloat16)

    pltpu.make_async_copy(part.at[pl.ds(0, n - 1)], part.at[pl.ds(0, n - 1)], part_send).wait()

    @pl.when(my_z == 0)
    def _():
        pltpu.make_async_copy(scales.at[pl.ds(0, n - 1)], scales.at[pl.ds(0, n - 1)], fin_send).wait()

    @pl.when(my_z > 0)
    def _():
        pltpu.make_async_copy(scales.at[pl.ds(0, nz - 1)], scales.at[pl.ds(0, nz - 1)], fin_send).wait()

    sides = pl.ds(0, (NY - 1) * (nz - 1))
    pltpu.make_async_copy(scales.at[sides], scales.at[sides], side_send).wait()
    pltpu.make_async_copy(rrecv.at[pl.ds(0, n - 1)], rrecv.at[pl.ds(0, n - 1)], r_send).wait()
    pltpu.make_async_copy(brecv.at[pl.ds(0, nb - 1)], brecv.at[pl.ds(0, nb - 1)], b_send).wait()
    for c in range(chunks):
        pltpu.make_async_copy(send.at[c, pl.ds(0, n - 1)], send.at[c, pl.ds(0, n - 1)], main_send.at[c]).wait()


def store(*refs):
    arrays = len(refs) // 2
    ins, outs, sem = refs[:arrays], refs[arrays : 2 * arrays], refs[-1]
    copies = [pltpu.make_async_copy(i, o, sem.at[k]) for k, (i, o) in enumerate(zip(ins, outs))]
    for copy in copies:
        copy.start()
    for copy in copies:
        copy.wait()


def solution(mesh):
    n, nb = mesh.shape["zero"], mesh.shape["bank"]

    def on_device(train_gate, other_gate, train_up, other_up, router_weight, router_gain):
        experts, rows, cols = train_gate.shape
        wide, lanes, chunks = cols // n, 2 * rows, experts
        f32, bf16 = jnp.float32, jnp.bfloat16
        hbm, vmem = pl.BlockSpec(memory_space=pltpu.HBM), pl.BlockSpec(memory_space=pltpu.VMEM)
        dma = pltpu.SemaphoreType.DMA
        shapes = (
            jax.ShapeDtypeStruct((experts, wide, rows * n), bf16),
            jax.ShapeDtypeStruct((experts, wide, rows * n), bf16),
            jax.ShapeDtypeStruct((experts, wide), f32),
            jax.ShapeDtypeStruct((experts, wide), f32),
            jax.ShapeDtypeStruct((rows * n, experts * nb), bf16),
        )
        held = pl.pallas_call(
            functools.partial(kernel, n, nb),
            out_shape=tuple(pltpu.VMEM(a.shape, a.dtype) for a in shapes),
            in_specs=[hbm] * 6,
            out_specs=(vmem,) * 5,
            scratch_shapes=[
                pltpu.VMEM((experts, rows, cols), f32),
                pltpu.VMEM((experts, rows, cols), bf16),
                pltpu.VMEM((experts, rows, cols), f32),
                pltpu.VMEM((experts, rows, cols), bf16),
                pltpu.VMEM((experts, rows), f32),
                pltpu.VMEM((1, rows), f32),
                pltpu.VMEM((n, 1, cols), f32),
                pltpu.VMEM((n, 1, cols), f32),
                pltpu.VMEM((1, 1, cols), f32),
                pltpu.VMEM((n, 1, cols), f32),
                pltpu.VMEM((cols, lanes), f32),
                pltpu.VMEM((chunks, n, wide, lanes), bf16),
                pltpu.VMEM((chunks, n, wide, lanes), bf16),
                pltpu.VMEM((experts // 2, lanes), bf16),
                pltpu.VMEM((n, experts // 2, lanes), bf16),
                pltpu.VMEM((n // 2, experts, lanes), bf16),
                pltpu.VMEM((nb, n // 2, experts, lanes), bf16),
                dma((4, chunks)),
                dma((2,)),
                dma, dma,
                dma, dma((n,)),
                dma, dma((NY,)),
                dma((chunks,)), dma((chunks,)),
                dma, dma,
                dma, dma,
            ],
            compiler_params=pltpu.CompilerParams(
                collective_id=0, has_side_effects=True, vmem_limit_bytes=40 << 20
            ),
        )(
            *(
                pltpu.with_memory_space_constraint(a, pltpu.HBM)
                for a in (train_gate, other_gate, train_up, other_up, router_weight.T, router_gain[None, :])
            )
        )
        out_g, out_u, sc_g, sc_u, router = pl.pallas_call(
            store,
            out_shape=shapes,
            in_specs=[vmem] * 5,
            out_specs=(hbm,) * 5,
            scratch_shapes=[dma((5,))],
            compiler_params=pltpu.CompilerParams(vmem_limit_bytes=4 << 20),
        )(*held)
        return jnp.swapaxes(out_g, 1, 2), jnp.swapaxes(out_u, 1, 2), sc_g, sc_u, router

    return jax.shard_map(
        on_device,
        mesh=mesh,
        in_specs=(
            P("bank", "zero", None),
            P("bank", "zero", None),
            P("bank", "zero", None),
            P("bank", "zero", None),
            P("zero", "bank"),
            P("zero"),
        ),
        out_specs=(
            P("bank", None, "zero"),
            P("bank", None, "zero"),
            P("bank", "zero"),
            P("bank", "zero"),
            P(),
        ),
        check_vma=False,
    )
```

```python
import functools

import jax
import jax.numpy as jnp
from jax import lax
from jax.experimental import pallas as pl
from jax.experimental.pallas import tpu as pltpu
from jax.sharding import PartitionSpec as P

MESH = pl.DeviceIdType.MESH
NY = 4


def kernel(
    n, nb,
    tg, og, tu, ou, rw, rg,
    out_gv, out_uv, sc_g, sc_u, routerv,
    tgv, ogv, tuv, ouv, rwv, rgv, part, gath, fin, scales, turned, send, recv,
    rsend, rrecv, bsend, brecv,
    in_sem, rw_sem, part_send, part_recv, fin_send, fin_recv, side_send, side_recv, main_send, main_recv,
    r_send, r_recv, b_send, b_recv,
):
    experts, rows, cols = tgv.shape
    chunks = experts
    wide = cols // n
    lanes = 2 * rows
    half = experts // 2
    me = lax.axis_index("zero")
    bank = lax.axis_index("bank")

    def mate_of(k):
        p = bank + k
        return jnp.where(p >= nb, p - nb, p)

    my_z = lax.div(me, NY)
    my_y = me - my_z * NY
    nz = n // NY

    def peer_of(k):
        z, y = my_z + k // NY, my_y + k % NY
        return jnp.where(z >= nz, z - nz, z) * NY + jnp.where(y >= NY, y - NY, y)

    def place(r):
        return r % NY * nz + r // NY

    def hops(k):
        return min(k // NY, nz - k // NY), min(k % NY, NY - k % NY)

    offsets = sorted(range(1, n), key=lambda k: (-hops(k)[0], -hops(k)[1]))
    strides = sorted(range(1, nb), key=lambda k: -min(k, nb - k))

    def load(c):
        at = pl.ds(c, 1)
        return [
            pltpu.make_async_copy(src.at[at], dst.at[at], in_sem.at[i, c])
            for i, (src, dst) in enumerate(((tg, tgv), (og, ogv), (tu, tuv), (ou, ouv)))
        ]

    for copy in load(0):
        copy.start()

    barrier = pltpu.get_barrier_semaphore()

    for k in offsets:
        pl.semaphore_signal(barrier, inc=1, device_id={"zero": peer_of(k)}, device_id_type=MESH)

    for k in strides:
        pl.semaphore_signal(barrier, inc=1, device_id={"bank": mate_of(k)}, device_id_type=MESH)

    for c in range(1, chunks):
        for copy in load(c):
            copy.start()

    rw_loads = (pltpu.make_async_copy(rw, rwv, rw_sem.at[0]), pltpu.make_async_copy(rg, rgv, rw_sem.at[1]))
    for copy in rw_loads:
        copy.start()

    def send_part(row):
        return pltpu.make_async_remote_copy(
            src_ref=part.at[row], dst_ref=gath.at[me], send_sem=part_send, recv_sem=part_recv,
            device_id={"zero": row}, device_id_type=MESH,
        )

    def largest(c):
        for copy in load(c):
            copy.wait()
        for kind, (t, o) in enumerate(((tgv, ogv), (tuv, ouv))):
            latest = t[c] + o[c].astype(jnp.float32)
            part[2 * c + kind] = jnp.max(jnp.abs(latest), axis=0, keepdims=True)

    def pass_on(c):
        for row in (2 * c, 2 * c + 1):

            @pl.when(row != me)
            def _():
                send_part(row).start()

    largest(0)
    pl.semaphore_wait(barrier, n - 1 + nb - 1)
    pass_on(0)

    @pl.loop(1, chunks)
    def _(c):
        largest(c)
        pass_on(c)

    gath[me] = part[me]

    for copy in rw_loads:
        copy.wait()
    block = rwv[...] * rgv[...]
    rsend[...] = jnp.concatenate([block[:half], block[half:]], axis=1).astype(jnp.bfloat16)

    for k in offsets:
        pltpu.make_async_remote_copy(
            src_ref=rsend, dst_ref=rrecv.at[me], send_sem=r_send, recv_sem=r_recv,
            device_id={"zero": peer_of(k)}, device_id_type=MESH,
        ).start()

    rrecv[me] = rsend[...]

    pltpu.make_async_copy(gath.at[pl.ds(0, n - 1)], gath.at[pl.ds(0, n - 1)], part_recv).wait()
    total = gath[0]
    for k in range(1, n):
        total = jnp.maximum(total, gath[k])
    fin[0] = total
    scales[my_y * nz + my_z] = total

    def send_fin(peer):
        return pltpu.make_async_remote_copy(
            src_ref=fin.at[0], dst_ref=scales.at[my_y * nz + my_z], send_sem=fin_send, recv_sem=fin_recv.at[me],
            device_id={"zero": peer}, device_id_type=MESH,
        )

    @pl.when(my_z == 0)
    def _():
        for k in offsets:
            send_fin(peer_of(k)).start()

    @pl.when(my_z > 0)
    def _():
        for k in sorted(range(1, nz), key=lambda k: -min(k, nz - k)):
            send_fin(peer_of(k * NY)).start()

    def take_fin(row, at):
        pltpu.make_async_copy(scales.at[at], scales.at[at], fin_recv.at[row]).wait()

    def take_first(r):
        @pl.when(me != r)
        def _():
            take_fin(r, place(r))

    def make(c):
        y, z = lax.rem(2 * c, NY), lax.div(2 * c, NY)
        inv_g = 1.0 / scales[y * nz + z]
        inv_u = 1.0 / scales[(y + 1) * nz + z]
        for b in range(cols // 128):
            at = slice(b * 128, (b + 1) * 128)
            gate = (tgv[c, :, at] + ogv[c, :, at].astype(jnp.float32)) * inv_g[:, at]
            up = (tuv[c, :, at] + ouv[c, :, at].astype(jnp.float32)) * inv_u[:, at]
            turned[at, :] = jnp.concatenate([gate, up], axis=0).T
        for p in range(n):
            send[c, p] = turned[p * wide : (p + 1) * wide, :].astype(jnp.bfloat16)
        recv[c, me] = send[c, me]

    def give(c, k):
        p = peer_of(k)
        pltpu.make_async_remote_copy(
            src_ref=send.at[c, p], dst_ref=recv.at[c, me], send_sem=main_send.at[c], recv_sem=main_recv.at[c],
            device_id={"zero": p}, device_id_type=MESH,
        ).start()

    def post(c):
        make(c)
        for k in offsets:
            give(c, k)

    def send_rows(k):
        at = pl.ds(my_y * nz + 1, nz - 1)
        return pltpu.make_async_remote_copy(
            src_ref=scales.at[at], dst_ref=scales.at[at], send_sem=side_send, recv_sem=side_recv.at[my_y],
            device_id={"zero": peer_of(k)}, device_id_type=MESH,
        )

    take_first(0)
    take_first(1)
    post(0)
    take_first(2)
    take_first(3)
    for z in range(1, nz):

        @pl.when(my_z != z)
        def _():
            take_fin(z * NY + my_y, my_y * nz + z)

    for k in range(1, NY):
        send_rows(k).start()
    post(1)
    for y in range(NY):

        @pl.when(my_y != y)
        def _():
            at = pl.ds(y * nz + 1, nz - 1)
            pltpu.make_async_copy(scales.at[at], scales.at[at], side_recv.at[y]).wait()

    pl.loop(2, chunks - 10)(post)
    pl.loop(chunks - 10, chunks)(make)
    for k in offsets:
        for c in range(chunks - 10, chunks):
            give(c, k)

    pltpu.make_async_copy(rrecv.at[pl.ds(0, n - 1)], rrecv.at[pl.ds(0, n - 1)], r_recv).wait()
    low = lax.broadcasted_iota(jnp.int32, (half, lanes), 1) < rows

    @pl.loop(0, n // 2)
    def _(k):
        a = rrecv[2 * k].astype(jnp.float32)
        b = rrecv[2 * k + 1].astype(jnp.float32)
        first = jnp.where(low, a, pltpu.roll(b, rows, 1))
        second = jnp.where(low, pltpu.roll(a, rows, 1), b)
        pair = jnp.concatenate([first, second], axis=0).astype(jnp.bfloat16)
        bsend[k] = pair
        brecv[bank, k] = pair

    for k in strides:
        pltpu.make_async_remote_copy(
            src_ref=bsend, dst_ref=brecv.at[bank], send_sem=b_send, recv_sem=b_recv,
            device_id={"bank": mate_of(k)}, device_id_type=MESH,
        ).start()

    for scv, kind in ((sc_g, 0), (sc_u, 1)):
        table = jnp.concatenate([scales[place(2 * e + kind)] for e in range(experts)], axis=0)
        scv[...] = pltpu.roll(table, (cols - wide * me) % cols, 1)[:, :wide]

    pltpu.make_async_copy(brecv.at[pl.ds(0, nb - 1)], brecv.at[pl.ds(0, nb - 1)], b_recv).wait()

    @pl.loop(0, n // 2)
    def _(k):
        tall = jnp.concatenate([brecv[b, k].astype(jnp.float32) for b in range(nb)], axis=0)
        routerv[pl.ds(pl.multiple_of(k * lanes, lanes), lanes), :] = tall.T.astype(jnp.bfloat16)

    side = lax.broadcasted_iota(jnp.int32, (wide, lanes), 1) < rows

    @pl.loop(0, chunks)
    def _(c):
        pltpu.make_async_copy(recv.at[c, pl.ds(0, n - 1)], recv.at[c, pl.ds(0, n - 1)], main_recv.at[c]).wait()
        for k in range(n // 2):
            a = recv[c, 2 * k].astype(jnp.float32)
            b = recv[c, 2 * k + 1].astype(jnp.float32)
            gate = jnp.where(side, a, pltpu.roll(b, rows, 1))
            up = jnp.where(side, pltpu.roll(a, rows, 1), b)
            out_gv[c, :, k * lanes : (k + 1) * lanes] = gate.astype(jnp.bfloat16)
            out_uv[c, :, k * lanes : (k + 1) * lanes] = up.astype(jnp.bfloat16)

    pltpu.make_async_copy(part.at[pl.ds(0, n - 1)], part.at[pl.ds(0, n - 1)], part_send).wait()

    @pl.when(my_z == 0)
    def _():
        pltpu.make_async_copy(scales.at[pl.ds(0, n - 1)], scales.at[pl.ds(0, n - 1)], fin_send).wait()

    @pl.when(my_z > 0)
    def _():
        pltpu.make_async_copy(scales.at[pl.ds(0, nz - 1)], scales.at[pl.ds(0, nz - 1)], fin_send).wait()

    sides = pl.ds(0, (NY - 1) * (nz - 1))
    pltpu.make_async_copy(scales.at[sides], scales.at[sides], side_send).wait()
    pltpu.make_async_copy(rrecv.at[pl.ds(0, n - 1)], rrecv.at[pl.ds(0, n - 1)], r_send).wait()
    pltpu.make_async_copy(brecv.at[pl.ds(0, nb - 1)], brecv.at[pl.ds(0, nb - 1)], b_send).wait()
    for c in range(chunks):
        pltpu.make_async_copy(send.at[c, pl.ds(0, n - 1)], send.at[c, pl.ds(0, n - 1)], main_send.at[c]).wait()


def store(*refs):
    arrays = len(refs) // 2
    ins, outs, sem = refs[:arrays], refs[arrays : 2 * arrays], refs[-1]
    copies = [pltpu.make_async_copy(i, o, sem.at[k]) for k, (i, o) in enumerate(zip(ins, outs))]
    for copy in copies:
        copy.start()
    for copy in copies:
        copy.wait()


def solution(mesh):
    n, nb = mesh.shape["zero"], mesh.shape["bank"]

    def on_device(train_gate, other_gate, train_up, other_up, router_weight, router_gain):
        experts, rows, cols = train_gate.shape
        wide, lanes, chunks = cols // n, 2 * rows, experts
        f32, bf16 = jnp.float32, jnp.bfloat16
        hbm, vmem = pl.BlockSpec(memory_space=pltpu.HBM), pl.BlockSpec(memory_space=pltpu.VMEM)
        dma = pltpu.SemaphoreType.DMA
        shapes = (
            jax.ShapeDtypeStruct((experts, wide, rows * n), bf16),
            jax.ShapeDtypeStruct((experts, wide, rows * n), bf16),
            jax.ShapeDtypeStruct((experts, wide), f32),
            jax.ShapeDtypeStruct((experts, wide), f32),
            jax.ShapeDtypeStruct((rows * n, experts * nb), bf16),
        )
        held = pl.pallas_call(
            functools.partial(kernel, n, nb),
            out_shape=tuple(pltpu.VMEM(a.shape, a.dtype) for a in shapes),
            in_specs=[hbm] * 6,
            out_specs=(vmem,) * 5,
            scratch_shapes=[
                pltpu.VMEM((experts, rows, cols), f32),
                pltpu.VMEM((experts, rows, cols), bf16),
                pltpu.VMEM((experts, rows, cols), f32),
                pltpu.VMEM((experts, rows, cols), bf16),
                pltpu.VMEM((experts, rows), f32),
                pltpu.VMEM((1, rows), f32),
                pltpu.VMEM((n, 1, cols), f32),
                pltpu.VMEM((n, 1, cols), f32),
                pltpu.VMEM((1, 1, cols), f32),
                pltpu.VMEM((n, 1, cols), f32),
                pltpu.VMEM((cols, lanes), f32),
                pltpu.VMEM((chunks, n, wide, lanes), bf16),
                pltpu.VMEM((chunks, n, wide, lanes), bf16),
                pltpu.VMEM((experts // 2, lanes), bf16),
                pltpu.VMEM((n, experts // 2, lanes), bf16),
                pltpu.VMEM((n // 2, experts, lanes), bf16),
                pltpu.VMEM((nb, n // 2, experts, lanes), bf16),
                dma((4, chunks)),
                dma((2,)),
                dma, dma,
                dma, dma((n,)),
                dma, dma((NY,)),
                dma((chunks,)), dma((chunks,)),
                dma, dma,
                dma, dma,
            ],
            compiler_params=pltpu.CompilerParams(
                collective_id=0, has_side_effects=True, vmem_limit_bytes=40 << 20
            ),
        )(
            *(
                pltpu.with_memory_space_constraint(a, pltpu.HBM)
                for a in (train_gate, other_gate, train_up, other_up, router_weight.T, router_gain[None, :])
            )
        )
        out_g, out_u, sc_g, sc_u, router = pl.pallas_call(
            store,
            out_shape=shapes,
            in_specs=[vmem] * 5,
            out_specs=(hbm,) * 5,
            scratch_shapes=[dma((5,))],
            compiler_params=pltpu.CompilerParams(vmem_limit_bytes=4 << 20),
        )(*held)
        return jnp.swapaxes(out_g, 1, 2), jnp.swapaxes(out_u, 1, 2), sc_g, sc_u, router

    return jax.shard_map(
        on_device,
        mesh=mesh,
        in_specs=(
            P("bank", "zero", None),
            P("bank", "zero", None),
            P("bank", "zero", None),
            P("bank", "zero", None),
            P("zero", "bank"),
            P("zero"),
        ),
        out_specs=(
            P("bank", None, "zero"),
            P("bank", None, "zero"),
            P("bank", "zero"),
            P("bank", "zero"),
            P(),
        ),
        check_vma=False,
    )
```

```python
import functools

import jax
import jax.numpy as jnp
from jax import lax
from jax.experimental import pallas as pl
from jax.experimental.pallas import tpu as pltpu
from jax.sharding import PartitionSpec as P

MESH = pl.DeviceIdType.MESH
NY = 4


def kernel(
    n, nb,
    tg, og, tu, ou, rw, rg,
    out_gv, out_uv, sc_g, sc_u, routerv,
    tgv, ogv, tuv, ouv, rwv, rgv, part, gath, fin, scales, turned, send, recv,
    rsend, rrecv, bsend, brecv,
    in_sem, rw_sem, part_send, part_recv, fin_send, fin_recv, side_send, side_recv, main_send, main_recv,
    r_send, r_recv, b_send, b_recv,
):
    experts, rows, cols = tgv.shape
    chunks = experts
    wide = cols // n
    lanes = 2 * rows
    half = experts // 2
    me = lax.axis_index("zero")
    bank = lax.axis_index("bank")

    def mate_of(k):
        p = bank + k
        return jnp.where(p >= nb, p - nb, p)

    my_z = lax.div(me, NY)
    my_y = me - my_z * NY
    nz = n // NY

    def peer_of(k):
        z, y = my_z + k // NY, my_y + k % NY
        return jnp.where(z >= nz, z - nz, z) * NY + jnp.where(y >= NY, y - NY, y)

    def place(r):
        return r % NY * nz + r // NY

    def hops(k):
        return min(k // NY, nz - k // NY), min(k % NY, NY - k % NY)

    offsets = sorted(range(1, n), key=lambda k: (-hops(k)[0], -hops(k)[1]))
    strides = sorted(range(1, nb), key=lambda k: -min(k, nb - k))

    def load(c):
        at = pl.ds(c, 1)
        return [
            pltpu.make_async_copy(src.at[at], dst.at[at], in_sem.at[i, c])
            for i, (src, dst) in enumerate(((tg, tgv), (og, ogv), (tu, tuv), (ou, ouv)))
        ]

    for copy in load(0):
        copy.start()

    barrier = pltpu.get_barrier_semaphore()

    for k in offsets:
        pl.semaphore_signal(barrier, inc=1, device_id={"zero": peer_of(k)}, device_id_type=MESH)

    for k in strides:
        pl.semaphore_signal(barrier, inc=1, device_id={"bank": mate_of(k)}, device_id_type=MESH)

    for c in range(1, chunks):
        for copy in load(c):
            copy.start()

    rw_loads = (pltpu.make_async_copy(rw, rwv, rw_sem.at[0]), pltpu.make_async_copy(rg, rgv, rw_sem.at[1]))
    for copy in rw_loads:
        copy.start()

    def send_part(row):
        return pltpu.make_async_remote_copy(
            src_ref=part.at[row], dst_ref=gath.at[me], send_sem=part_send, recv_sem=part_recv,
            device_id={"zero": row}, device_id_type=MESH,
        )

    def largest(c):
        for copy in load(c):
            copy.wait()
        for kind, (t, o) in enumerate(((tgv, ogv), (tuv, ouv))):
            latest = t[c] + o[c].astype(jnp.float32)
            part[2 * c + kind] = jnp.max(jnp.abs(latest), axis=0, keepdims=True)

    def pass_on(c):
        for row in (2 * c, 2 * c + 1):

            @pl.when(row != me)
            def _():
                send_part(row).start()

    largest(0)
    pl.semaphore_wait(barrier, n - 1 + nb - 1)
    pass_on(0)

    @pl.loop(1, chunks)
    def _(c):
        largest(c)

        @pl.when(c > 1)
        def _():
            pass_on(c - 1)

    pass_on(chunks - 1)

    gath[me] = part[me]

    for copy in rw_loads:
        copy.wait()
    block = rwv[...] * rgv[...]
    rsend[...] = jnp.concatenate([block[:half], block[half:]], axis=1).astype(jnp.bfloat16)

    for k in offsets:
        pltpu.make_async_remote_copy(
            src_ref=rsend, dst_ref=rrecv.at[me], send_sem=r_send, recv_sem=r_recv,
            device_id={"zero": peer_of(k)}, device_id_type=MESH,
        ).start()

    rrecv[me] = rsend[...]

    pltpu.make_async_copy(gath.at[pl.ds(0, n - 1)], gath.at[pl.ds(0, n - 1)], part_recv).wait()
    total = gath[0]
    for k in range(1, n):
        total = jnp.maximum(total, gath[k])
    fin[0] = total
    scales[my_y * nz + my_z] = total

    def send_fin(peer):
        return pltpu.make_async_remote_copy(
            src_ref=fin.at[0], dst_ref=scales.at[my_y * nz + my_z], send_sem=fin_send, recv_sem=fin_recv.at[me],
            device_id={"zero": peer}, device_id_type=MESH,
        )

    @pl.when(my_z == 0)
    def _():
        for k in offsets:
            send_fin(peer_of(k)).start()

    @pl.when(my_z > 0)
    def _():
        for k in sorted(range(1, nz), key=lambda k: -min(k, nz - k)):
            send_fin(peer_of(k * NY)).start()

    def take_fin(row, at):
        pltpu.make_async_copy(scales.at[at], scales.at[at], fin_recv.at[row]).wait()

    def take_first(r):
        @pl.when(me != r)
        def _():
            take_fin(r, place(r))

    def make(c):
        y, z = lax.rem(2 * c, NY), lax.div(2 * c, NY)
        inv_g = 1.0 / scales[y * nz + z]
        inv_u = 1.0 / scales[(y + 1) * nz + z]
        for b in range(cols // 128):
            at = slice(b * 128, (b + 1) * 128)
            gate = (tgv[c, :, at] + ogv[c, :, at].astype(jnp.float32)) * inv_g[:, at]
            up = (tuv[c, :, at] + ouv[c, :, at].astype(jnp.float32)) * inv_u[:, at]
            turned[at, :] = jnp.concatenate([gate, up], axis=0).T
        for p in range(n):
            send[c, p] = turned[p * wide : (p + 1) * wide, :].astype(jnp.bfloat16)
        recv[c, me] = send[c, me]

    def give(c, k):
        p = peer_of(k)
        pltpu.make_async_remote_copy(
            src_ref=send.at[c, p], dst_ref=recv.at[c, me], send_sem=main_send.at[c], recv_sem=main_recv.at[c],
            device_id={"zero": p}, device_id_type=MESH,
        ).start()

    def post(c):
        make(c)
        for k in offsets:
            give(c, k)

    def send_rows(k):
        at = pl.ds(my_y * nz + 1, nz - 1)
        return pltpu.make_async_remote_copy(
            src_ref=scales.at[at], dst_ref=scales.at[at], send_sem=side_send, recv_sem=side_recv.at[my_y],
            device_id={"zero": peer_of(k)}, device_id_type=MESH,
        )

    take_first(0)
    take_first(1)
    post(0)
    take_first(2)
    take_first(3)
    for z in range(1, nz):

        @pl.when(my_z != z)
        def _():
            take_fin(z * NY + my_y, my_y * nz + z)

    for k in range(1, NY):
        send_rows(k).start()
    post(1)
    for y in range(NY):

        @pl.when(my_y != y)
        def _():
            at = pl.ds(y * nz + 1, nz - 1)
            pltpu.make_async_copy(scales.at[at], scales.at[at], side_recv.at[y]).wait()

    pl.loop(2, chunks - 10)(make)
    for k in offsets:
        for c in range(2, chunks - 10):
            give(c, k)
    pl.loop(chunks - 10, chunks)(make)
    for k in offsets:
        for c in range(chunks - 10, chunks):
            give(c, k)

    pltpu.make_async_copy(rrecv.at[pl.ds(0, n - 1)], rrecv.at[pl.ds(0, n - 1)], r_recv).wait()
    low = lax.broadcasted_iota(jnp.int32, (half, lanes), 1) < rows

    @pl.loop(0, n // 2)
    def _(k):
        a = rrecv[2 * k].astype(jnp.float32)
        b = rrecv[2 * k + 1].astype(jnp.float32)
        first = jnp.where(low, a, pltpu.roll(b, rows, 1))
        second = jnp.where(low, pltpu.roll(a, rows, 1), b)
        pair = jnp.concatenate([first, second], axis=0).astype(jnp.bfloat16)
        bsend[k] = pair
        brecv[bank, k] = pair

    for k in strides:
        pltpu.make_async_remote_copy(
            src_ref=bsend, dst_ref=brecv.at[bank], send_sem=b_send, recv_sem=b_recv,
            device_id={"bank": mate_of(k)}, device_id_type=MESH,
        ).start()

    for scv, kind in ((sc_g, 0), (sc_u, 1)):
        table = jnp.concatenate([scales[place(2 * e + kind)] for e in range(experts)], axis=0)
        scv[...] = pltpu.roll(table, (cols - wide * me) % cols, 1)[:, :wide]

    pltpu.make_async_copy(brecv.at[pl.ds(0, nb - 1)], brecv.at[pl.ds(0, nb - 1)], b_recv).wait()

    @pl.loop(0, n // 2)
    def _(k):
        tall = jnp.concatenate([brecv[b, k].astype(jnp.float32) for b in range(nb)], axis=0)
        routerv[pl.ds(pl.multiple_of(k * lanes, lanes), lanes), :] = tall.T.astype(jnp.bfloat16)

    side = lax.broadcasted_iota(jnp.int32, (wide, lanes), 1) < rows

    @pl.loop(0, chunks)
    def _(c):
        pltpu.make_async_copy(recv.at[c, pl.ds(0, n - 1)], recv.at[c, pl.ds(0, n - 1)], main_recv.at[c]).wait()
        for k in range(n // 2):
            a = recv[c, 2 * k].astype(jnp.float32)
            b = recv[c, 2 * k + 1].astype(jnp.float32)
            gate = jnp.where(side, a, pltpu.roll(b, rows, 1))
            up = jnp.where(side, pltpu.roll(a, rows, 1), b)
            out_gv[c, :, k * lanes : (k + 1) * lanes] = gate.astype(jnp.bfloat16)
            out_uv[c, :, k * lanes : (k + 1) * lanes] = up.astype(jnp.bfloat16)

    pltpu.make_async_copy(part.at[pl.ds(0, n - 1)], part.at[pl.ds(0, n - 1)], part_send).wait()

    @pl.when(my_z == 0)
    def _():
        pltpu.make_async_copy(scales.at[pl.ds(0, n - 1)], scales.at[pl.ds(0, n - 1)], fin_send).wait()

    @pl.when(my_z > 0)
    def _():
        pltpu.make_async_copy(scales.at[pl.ds(0, nz - 1)], scales.at[pl.ds(0, nz - 1)], fin_send).wait()

    sides = pl.ds(0, (NY - 1) * (nz - 1))
    pltpu.make_async_copy(scales.at[sides], scales.at[sides], side_send).wait()
    pltpu.make_async_copy(rrecv.at[pl.ds(0, n - 1)], rrecv.at[pl.ds(0, n - 1)], r_send).wait()
    pltpu.make_async_copy(brecv.at[pl.ds(0, nb - 1)], brecv.at[pl.ds(0, nb - 1)], b_send).wait()
    for c in range(chunks):
        pltpu.make_async_copy(send.at[c, pl.ds(0, n - 1)], send.at[c, pl.ds(0, n - 1)], main_send.at[c]).wait()


def store(*refs):
    arrays = len(refs) // 2
    ins, outs, sem = refs[:arrays], refs[arrays : 2 * arrays], refs[-1]
    copies = [pltpu.make_async_copy(i, o, sem.at[k]) for k, (i, o) in enumerate(zip(ins, outs))]
    for copy in copies:
        copy.start()
    for copy in copies:
        copy.wait()


def solution(mesh):
    n, nb = mesh.shape["zero"], mesh.shape["bank"]

    def on_device(train_gate, other_gate, train_up, other_up, router_weight, router_gain):
        experts, rows, cols = train_gate.shape
        wide, lanes, chunks = cols // n, 2 * rows, experts
        f32, bf16 = jnp.float32, jnp.bfloat16
        hbm, vmem = pl.BlockSpec(memory_space=pltpu.HBM), pl.BlockSpec(memory_space=pltpu.VMEM)
        dma = pltpu.SemaphoreType.DMA
        shapes = (
            jax.ShapeDtypeStruct((experts, wide, rows * n), bf16),
            jax.ShapeDtypeStruct((experts, wide, rows * n), bf16),
            jax.ShapeDtypeStruct((experts, wide), f32),
            jax.ShapeDtypeStruct((experts, wide), f32),
            jax.ShapeDtypeStruct((rows * n, experts * nb), bf16),
        )
        held = pl.pallas_call(
            functools.partial(kernel, n, nb),
            out_shape=tuple(pltpu.VMEM(a.shape, a.dtype) for a in shapes),
            in_specs=[hbm] * 6,
            out_specs=(vmem,) * 5,
            scratch_shapes=[
                pltpu.VMEM((experts, rows, cols), f32),
                pltpu.VMEM((experts, rows, cols), bf16),
                pltpu.VMEM((experts, rows, cols), f32),
                pltpu.VMEM((experts, rows, cols), bf16),
                pltpu.VMEM((experts, rows), f32),
                pltpu.VMEM((1, rows), f32),
                pltpu.VMEM((n, 1, cols), f32),
                pltpu.VMEM((n, 1, cols), f32),
                pltpu.VMEM((1, 1, cols), f32),
                pltpu.VMEM((n, 1, cols), f32),
                pltpu.VMEM((cols, lanes), f32),
                pltpu.VMEM((chunks, n, wide, lanes), bf16),
                pltpu.VMEM((chunks, n, wide, lanes), bf16),
                pltpu.VMEM((experts // 2, lanes), bf16),
                pltpu.VMEM((n, experts // 2, lanes), bf16),
                pltpu.VMEM((n // 2, experts, lanes), bf16),
                pltpu.VMEM((nb, n // 2, experts, lanes), bf16),
                dma((4, chunks)),
                dma((2,)),
                dma, dma,
                dma, dma((n,)),
                dma, dma((NY,)),
                dma((chunks,)), dma((chunks,)),
                dma, dma,
                dma, dma,
            ],
            compiler_params=pltpu.CompilerParams(
                collective_id=0, has_side_effects=True, vmem_limit_bytes=40 << 20
            ),
        )(
            *(
                pltpu.with_memory_space_constraint(a, pltpu.HBM)
                for a in (train_gate, other_gate, train_up, other_up, router_weight.T, router_gain[None, :])
            )
        )
        out_g, out_u, sc_g, sc_u, router = pl.pallas_call(
            store,
            out_shape=shapes,
            in_specs=[vmem] * 5,
            out_specs=(hbm,) * 5,
            scratch_shapes=[dma((5,))],
            compiler_params=pltpu.CompilerParams(vmem_limit_bytes=4 << 20),
        )(*held)
        return jnp.swapaxes(out_g, 1, 2), jnp.swapaxes(out_u, 1, 2), sc_g, sc_u, router

    return jax.shard_map(
        on_device,
        mesh=mesh,
        in_specs=(
            P("bank", "zero", None),
            P("bank", "zero", None),
            P("bank", "zero", None),
            P("bank", "zero", None),
            P("zero", "bank"),
            P("zero"),
        ),
        out_specs=(
            P("bank", None, "zero"),
            P("bank", None, "zero"),
            P("bank", "zero"),
            P("bank", "zero"),
            P(),
        ),
        check_vma=False,
    )
```
